32 devices in a mesh: member: 8 (over y, x, core), dp: 4 (over z).
Axes of the slice: x: 2, y: 2, z: 4, core: 2. Of those that a mesh axis runs over, the one named last changes fastest.
Arguments:
- trunk: bfloat16 [1576, 1024], P('dp'), may hold values from -6 to 6
- normgain: float32 [1024], replicated, may hold values from 0.25 to 1.75
- expand: bfloat16 [1024, 2048], P('member'), may hold values from -0.1875 to 0.1875
- shrink: bfloat16 [2048, 1024], P('member'), may hold values from -0.125 to 0.125
- inscale: float32 [8, 1024], P('member'), may hold values from 0.25 to 1.75
- hidscale: float32 [8, 2048], P('member'), may hold values from 0.25 to 1.75
- actscale: float32 [8, 2048], P('member'), may hold values from 0.25 to 1.75
- outscale: float32 [8, 1024], P('member'), may hold values from 0.25 to 1.75
- cotangent: bfloat16 [8, 1576, 1024], P('member', 'dp'), may hold values from -6 to 6
Outputs:
- trunk_grad: bfloat16 [1576, 1024], P('dp', 'member')
- expand_grad: float32 [1024, 2048], P('member')
- shrink_grad: float32 [2048, 1024], P('member')
- inscale_grad: float32 [8, 1024], P('member')
- hidscale_grad: float32 [8, 2048], P('member')
- actscale_grad: float32 [8, 2048], P('member')
- outscale_grad: float32 [8, 1024], P('member')
- normgain_grad: float32 [1024], replicated
The draws below stay inside these ranges and needn't reach their ends.
All inputs are finite; a program needn't handle non-finite values.
Results may differ from the reference program's by a relative error of at most 0.024.
Values may be sent and summed in bfloat16 or wider, within the bound.
A program may use at most 64 MiB of HBM per device.

```python
import jax
import jax.numpy as jnp
from jax import lax

D = 1024
FF = 2048
TOK_DEV = 394
TOKENS = 1576
MEMBERS = 8
N_DP = 4


def with_spikes(result, rng, source, target, parts, factor):
    owner, partner = [(jnp.arange(result.shape[axis_at]) // (result.shape[axis_at] // parts)).reshape([-1 if axis == axis_at else 1 for axis in range(result.ndim)]) for axis_at in (source, target)]
    chosen = jax.random.permutation(rng, parts)[partner]
    strong = (owner == chosen) | (owner == (partner + parts // 2) % parts)
    return jnp.where(strong, factor * result, result)


def level_of(rng, dims, cuts, least, high):
    level = 1.0
    for dim, parts in cuts:
        heights = jax.random.uniform(jax.random.fold_in(jax.random.fold_in(rng, 6), dim), (parts,), jnp.float32, least / len(cuts), high / len(cuts))
        level = level * jnp.repeat(jnp.exp(heights), dims[dim] // parts).reshape((-1,) + (1,) * (len(dims) - 1 - dim))
    return level


def centred(rng, shape, scale, bound, shards=(), kind=jnp.bfloat16):
    drawn = scale * jax.random.normal(rng, shape, jnp.float32)
    if shards:
        drawn = drawn * level_of(rng, shape, shards, -0.22, 0.18)
    return jnp.clip(drawn, -bound, bound).astype(kind)


def heavy_noise(key, dims, spread, reach, cuts, heavy, kind=jnp.bfloat16):
    values = spread * jax.random.normal(key, dims, jnp.float32)
    if cuts:
        values = values * level_of(key, dims, cuts, -0.22, 0.18)
    return jnp.clip(with_spikes(values, jax.random.fold_in(key, 3), *heavy), -reach, reach).astype(kind)


def setup_inputs(seed: int = 0) -> dict:
    seeds = jax.random.split(jax.random.key(seed), 10)
    return {
        "trunk": centred(seeds[0], (TOKENS, D), 1.0, 6.0, ((0, 4),)),
        "normgain": jnp.clip(1.0 + 0.15 * jax.random.normal(seeds[1], (D,), jnp.float32), 0.25, 1.75),
        "expand": centred(seeds[2], (D, FF), D ** -0.5, 0.1875, ((0, 8),)),
        "shrink": centred(seeds[3], (FF, D), FF ** -0.5, 0.125, ((0, 8),)),
        "inscale": jnp.clip(1.0 + 0.15 * jax.random.normal(seeds[4], (MEMBERS, D), jnp.float32), 0.25, 1.75),
        "hidscale": jnp.clip(1.0 + 0.15 * jax.random.normal(seeds[5], (MEMBERS, FF), jnp.float32), 0.25, 1.75),
        "actscale": jnp.clip(1.0 + 0.15 * jax.random.normal(seeds[6], (MEMBERS, FF), jnp.float32), 0.25, 1.75),
        "outscale": jnp.clip(1.0 + 0.15 * jax.random.normal(seeds[7], (MEMBERS, D), jnp.float32), 0.25, 1.75),
        "cotangent": heavy_noise(seeds[8], (MEMBERS, TOKENS, D), 1.0, 6.0, ((0, 8), (1, 4)), (0, 2, 8, 2.0)),
    }


eps = 1e-06
coeff = 0.7978845608028654

def gelu_pair(hidden):
    inner = coeff * (hidden + 0.044715 * hidden * hidden * hidden)
    tangent = jnp.tanh(inner)
    active = 0.5 * hidden * (1.0 + tangent)
    slope = 0.5 * (1.0 + tangent) + 0.5 * hidden * (1.0 - tangent * tangent) * coeff * (1.0 + 3.0 * 0.044715 * hidden * hidden)
    return (active, slope)

def block_terms(left, right):
    left_blocks = left.astype(jnp.float32).reshape(N_DP, TOK_DEV, left.shape[1])
    right_blocks = right.astype(jnp.float32).reshape(N_DP, TOK_DEV, right.shape[1])
    terms = jnp.einsum('bti,btj->bij', left_blocks, right_blocks, precision=lax.Precision.HIGHEST)
    rounded = lax.optimization_barrier(terms.astype(jnp.bfloat16))
    return lax.optimization_barrier(jnp.sum(rounded.astype(jnp.float32), axis=0))

def reference(trunk, normgain, expand, shrink, inscale, hidscale, actscale, outscale, cotangent):
    tokens = trunk.astype(jnp.float32)
    centered = tokens - lax.optimization_barrier(jnp.mean(tokens, axis=1, keepdims=True))
    variance = lax.optimization_barrier(jnp.mean(centered * centered, axis=1, keepdims=True))
    inv_std = lax.rsqrt(variance + eps)
    normed = centered * inv_std
    gained = normed * normgain

    def member_step(carry, pieces):
        trunk_acc, expand_acc, shrink_acc, gain_acc = carry
        scale_in, scale_hid, scale_act, scale_out, cot = pieces
        scaled_in = (gained * scale_in).astype(jnp.bfloat16)
        project = jnp.dot(scaled_in, expand, preferred_element_type=jnp.float32)
        hidden = project * scale_hid
        active, slope = gelu_pair(hidden)
        scaled_act = (active * scale_act).astype(jnp.bfloat16)
        second = jnp.dot(scaled_act, shrink, preferred_element_type=jnp.float32)
        upstream = cot.astype(jnp.float32)
        grad_out = lax.optimization_barrier(jnp.sum(upstream * second, axis=0))
        scaled_cot = (upstream * scale_out).astype(jnp.bfloat16)
        back_act = jnp.dot(scaled_cot, shrink.T, preferred_element_type=jnp.float32)
        grad_act = lax.optimization_barrier(jnp.sum(back_act * active, axis=0))
        back_hidden = back_act * scale_act * slope
        grad_hid = lax.optimization_barrier(jnp.sum(back_hidden * project, axis=0))
        back_proj = (back_hidden * scale_hid).astype(jnp.bfloat16)
        shrink_acc = shrink_acc + block_terms(scaled_act, scaled_cot)
        expand_acc = expand_acc + block_terms(scaled_in, back_proj)
        back_norm = jnp.dot(back_proj, expand.T, preferred_element_type=jnp.float32)
        grad_in = lax.optimization_barrier(jnp.sum(back_norm * gained, axis=0))
        back_scaled = back_norm * scale_in
        gain_acc = gain_acc + lax.optimization_barrier(jnp.sum(back_scaled * normed, axis=0))
        back_unit = back_scaled * normgain
        back_trunk = inv_std * (back_unit - lax.optimization_barrier(jnp.mean(back_unit, axis=1, keepdims=True)) - normed * lax.optimization_barrier(jnp.mean(back_unit * normed, axis=1, keepdims=True)))
        trunk_acc = trunk_acc + upstream + back_trunk
        return ((trunk_acc, expand_acc, shrink_acc, gain_acc), (grad_in, grad_hid, grad_act, grad_out))
    start = (jnp.zeros(tokens.shape, jnp.float32), jnp.zeros(expand.shape, jnp.float32), jnp.zeros(shrink.shape, jnp.float32), jnp.zeros(normgain.shape, jnp.float32))
    carry, grads = lax.scan(member_step, start, (inscale, hidscale, actscale, outscale, cotangent))
    trunk_acc, expand_acc, shrink_acc, gain_acc = carry
    grad_in, grad_hid, grad_act, grad_out = grads
    return (trunk_acc.astype(jnp.bfloat16), expand_acc, shrink_acc, grad_in, grad_hid, grad_act, grad_out, gain_acc)
```

```python
import functools

import jax
import jax.numpy as jnp
from jax import lax
from jax.experimental import pallas as pl
from jax.experimental.pallas import tpu as pltpu
from jax.sharding import PartitionSpec as P

eps = 1e-06
coeff = 0.7978845608028654
MESH = pl.DeviceIdType.MESH
F32, BF16 = jnp.float32, jnp.bfloat16
PARTS = (2, 2, 2, 2)
RELAY_AT = 5
VMEM_LIMIT = 64000 * 1024


def gelu_pair(hidden):
    inner = coeff * (hidden + 0.044715 * hidden * hidden * hidden)
    tangent = jnp.tanh(inner)
    active = 0.5 * hidden * (1.0 + tangent)
    slope = 0.5 * (1.0 + tangent) + 0.5 * hidden * (1.0 - tangent * tangent) * coeff * (
        1.0 + 3.0 * 0.044715 * hidden * hidden
    )
    return (active, slope)


def dot(a, b, da, db):
    return lax.dot_general(a, b, (((da,), (db,)), ((), ())), preferred_element_type=F32)


def kernel(
    n, nz,
    trunk, gain, expand, shrink, r_in, r_out, r_hid, r_act, cot,
    o_trunk, o_expand, o_shrink, o_small,
    scales, e_all, et, sc_all, cots, si_all, proj_all, act_all, slope_all, sa_all, normed_ref, inv_ref,
    b_acc, s_acc, e_acc, g_acc,
    e_send, e_recv, s_send, t_sum, u_send, u_recv, t_send, t_recv,
    s_in1, s_part, s_in2, s_fin, e_in1, e_part, e_in2, e_fin, t_in1, t_part, t_in2, t_fin,
    sem_es, sem_er, sem_ss, sem_sr, sem_cs, sem_cr, sem_fs, sem_ps,
    sem_gs, sem_gr, sem_us, sem_ur, sem_ts, sem_tr,
    sem_zs, sem_ze, sem_zt,
):
    me = lax.axis_index("member")
    mz = lax.axis_index("dp")
    tok, d = trunk.shape
    ff = expand.shape[1]
    fs = ff // n
    ds = d // n
    half = d // 2
    gy = 2
    gx = n // (2 * gy)
    core, xx, yy = me % 2, (me // 2) % gx, me // (2 * gx)

    def peer(s):
        c = (core + s % 2) % 2
        a = (xx + (s // 2) % gx) % gx
        b = (yy + s // (2 * gx)) % gy
        return (b * gx + a) * 2 + c

    def zpeer(k):
        return (mz + k) % nz

    def remote(src, dst, ss, rs, axis, who):
        return pltpu.make_async_remote_copy(
            src_ref=src, dst_ref=dst, send_sem=ss, recv_sem=rs,
            device_id={axis: who}, device_id_type=MESH,
        )

    scales[:, pl.ds(0, d)] = r_in[...]
    scales[:, pl.ds(d, d)] = r_out[...]
    scales[:, pl.ds(2 * d, ff)] = r_hid[...]
    scales[:, pl.ds(2 * d + ff, ff)] = r_act[...]

    barrier = pltpu.get_barrier_semaphore()
    for s in range(1, n):
        pl.semaphore_signal(barrier, inc=1, device_id={"member": peer(s)}, device_id_type=MESH)
    for k in range(1, nz):
        pl.semaphore_signal(barrier, inc=1, device_id={"dp": zpeer(k)}, device_id_type=MESH)
    pl.semaphore_wait(barrier, n - 1 + nz - 1)

    def e_cp(s):
        p = peer(s)
        return remote(
            expand.at[:, pl.ds(pl.multiple_of(p * fs, fs), fs)], e_all.at[me],
            sem_es.at[s], sem_er.at[me], "member", p)

    def sc_cp(s):
        return remote(scales, sc_all.at[me], sem_ss.at[s], sem_sr.at[me], "member", peer(s))

    def hs(h):
        return pl.ds(h * half, half)

    def own_cp(s, h):
        return remote(
            cot.at[:, hs(h)], cots.at[me, :, hs(h)], sem_cs.at[s, h], sem_cr.at[me, h],
            "member", peer(s))

    def fwd_cp(m, h, s, sem):
        return remote(
            cots.at[m, :, hs(h)], cots.at[m, :, hs(h)], sem, sem_cr.at[m, h], "member", peer(s))

    def cot_wait(m, h):
        fwd_cp(m, h, 1, sem_fs.at[0]).wait_recv()

    order = [s for s in range(2, n)] + [1]
    for s in order:
        sc_cp(s).start()
        e_cp(s).start()
    square = n == 8
    own_sends = [(1, 0), (1, 1)]
    if square:
        own_sends += [(2, 0), (4, 1), (2, 1), (4, 0)]
    else:
        own_sends += [(s, h) for s in range(2, n, 2) for h in range(2)]
    for s, h in own_sends:
        own_cp(s, h).start()

    e_all[me] = expand[:, pl.ds(pl.multiple_of(me * fs, fs), fs)]
    sc_all[me] = scales[...]
    cots[me] = cot[...]

    tokens = trunk[...].astype(F32)
    centered = tokens - jnp.mean(tokens, axis=1, keepdims=True)
    inv = lax.rsqrt(jnp.mean(centered * centered, axis=1, keepdims=True) + eps)
    normed_ref[...] = centered * inv
    inv_ref[...] = inv
    b_acc[...] = jnp.zeros_like(b_acc)
    s_acc[...] = jnp.zeros_like(s_acc)
    e_acc[...] = jnp.zeros_like(e_acc)
    g_acc[...] = jnp.zeros_like(g_acc)

    for s in order:
        p = peer(s)
        remote(scales, sc_all.at[p], sem_ss.at[s], sem_sr.at[p], "member", p).wait_recv()
        remote(e_all.at[p], e_all.at[p], sem_es.at[s], sem_er.at[p], "member", p).wait_recv()

    et[...] = e_all[...].reshape(d, fs).T

    def scale_rows(m):
        a = sc_all[m, :, pl.ds(0, d)]
        b = sc_all[m, :, pl.ds(d, d)]
        c = sc_all[m, :, pl.ds(pl.multiple_of(2 * d + me * fs, fs), fs)]
        e = sc_all[m, :, pl.ds(pl.multiple_of(2 * d + ff + me * fs, fs), fs)]
        return a, b, c, e

    @pl.loop(0, n)
    def _(s):
        m = peer(s)
        s_in, s_out, s_hid, s_act = scale_rows(m)
        si = (normed_ref[...] * gain[...] * s_in).astype(BF16)
        si_all[s] = si
        proj = dot(si, e_all[...].reshape(d, fs), 1, 0)
        active, slope = gelu_pair(proj * s_hid)
        proj_all[s] = proj
        act_all[s] = active
        slope_all[s] = slope * s_act
        sa_all[s] = (active * s_act).astype(BF16)

    @pl.loop(0, n)
    def _(s):
        m = peer(s)
        if square:
            @pl.when(s == 1)
            def _():
                cot_wait(peer(2), 0)
                fwd_cp(peer(2), 0, 4, sem_fs.at[0]).start()
                cot_wait(peer(4), 1)
                fwd_cp(peer(4), 1, 2, sem_fs.at[1]).start()

            @pl.when((s % 2 == 1) | (s == 6))
            def _():
                cot_wait(m, 0)
                cot_wait(m, 1)

            @pl.when(s == 2)
            def _():
                cot_wait(m, 1)

            @pl.when(s == 4)
            def _():
                cot_wait(m, 0)
        else:
            @pl.when(s > 0)
            def _():
                cot_wait(m, 0)
                cot_wait(m, 1)

        @pl.when((s % 2 == 0) & (s > 0))
        def _():
            for h in range(2):
                fwd_cp(m, h, 1, sem_ps.at[s, h]).start()

        s_in, s_out, s_hid, s_act = scale_rows(m)
        upstream = cots[m].astype(F32)
        scaled_cot = (upstream * s_out).astype(BF16)
        back_act = dot(scaled_cot, shrink[...], 1, 1)
        g_act = jnp.sum(back_act * act_all[s], axis=0, keepdims=True)
        back_hid = back_act * slope_all[s]
        g_hid = jnp.sum(back_hid * proj_all[s], axis=0, keepdims=True)
        back_proj = (back_hid * s_hid).astype(BF16)
        s_term = dot(sa_all[s], scaled_cot, 0, 0)
        s_acc[...] += s_term
        g_out = jnp.sum(s_term * shrink[...].astype(F32), axis=0, keepdims=True) / s_out
        e_term = dot(back_proj, si_all[s], 0, 0)
        e_acc[...] += e_term
        e_sum = jnp.sum(e_term * et[...].astype(F32), axis=0, keepdims=True)
        g_acc[...] += e_sum
        b_acc[...] += dot(back_proj, et[...], 1, 0) * s_in
        t_send[m, :, pl.ds(0, d)] = e_sum / s_in
        t_send[m, :, pl.ds(d, d)] = g_out
        t_send[m, :, pl.ds(3 * d, fs)] = g_hid
        t_send[m, :, pl.ds(3 * d + fs, fs)] = g_act

    chain = nz == 4
    inner = (mz == 1) | (mz == 2)
    outer = (mz == 0) | (mz == 3)
    pair = mz + 1 - 2 * (mz % 2)
    across = 3 - mz

    class Reduce:
        def __init__(self, own, in1, part, in2, fin, sem):
            self.refs, self.sem = (own, in1, part, in2, fin), sem

        def hop(self, k, q):
            own, in1, part, in2, fin = self.refs
            src, dst, who = ((own, in1, pair), (part, in2, across), (fin, fin, pair))[k]
            return remote(src.at[q], dst.at[q], self.sem.at[2 * k, q], self.sem.at[2 * k + 1, q], "dp", who)

        def start(self, q):
            if chain:
                @pl.when(outer)
                def _():
                    self.hop(0, q).start()

        def mid(self, q):
            own, in1, part, in2, fin = self.refs
            if chain:
                @pl.when(inner)
                def _():
                    self.hop(0, q).wait_recv()
                    part[q] = (own[q].astype(F32) + in1[q].astype(F32)).astype(part.dtype)
                    self.hop(1, q).start()

        def fin(self, q):
            own, in1, part, in2, fin = self.refs
            if chain:
                @pl.when(inner)
                def _():
                    self.hop(1, q).wait_recv()
                    fin[q] = (part[q].astype(F32) + in2[q].astype(F32)).astype(fin.dtype)
                    self.hop(2, q).start()

        def end(self, q):
            if chain:
                @pl.when(outer)
                def _():
                    self.hop(2, q).wait_recv()

        def sent(self, q):
            if chain:
                @pl.when(outer)
                def _():
                    self.hop(0, q).wait_send()

                @pl.when(inner)
                def _():
                    self.hop(1, q).wait_send()
                    self.hop(2, q).wait_send()

        def whole(self, k, slot):
            own, in1 = self.refs[:2]
            return remote(own, in1.at[slot], self.sem.at[0, k], self.sem.at[1, slot], "dp", zpeer(k))

        def plain(self):
            own, in1, part, in2, fin = self.refs
            for k in range(1, nz):
                self.whole(k, mz).start()
            in1[mz] = own[...]
            for k in range(1, nz):
                self.whole(k, zpeer(k)).wait_recv()
            fin[...] = sum(in1[z].astype(F32) for z in range(nz)).astype(fin.dtype)
            for k in range(1, nz):
                self.whole(k, mz).wait_send()

    red_s = Reduce(s_send, s_in1, s_part, s_in2, s_fin, sem_zs)
    red_e = Reduce(e_recv, e_in1, e_part, e_in2, e_fin, sem_ze)
    red_t = Reduce(t_sum, t_in1, t_part, t_in2, t_fin, sem_zt)

    rz = s_acc.shape[0] // nz
    for q in range(nz):
        s_send[q] = s_acc[pl.ds(q * rz, rz), :].astype(BF16)
        red_s.start(q)

    ez = ds // nz
    e_t = e_acc[...].T.astype(BF16)
    for p in range(n):
        for q in range(nz):
            e_send[p, q] = e_t[p * ds + q * ez:p * ds + (q + 1) * ez, :]
    for s in order:
        p = peer(s)
        remote(e_send.at[p], e_recv.at[:, me], sem_gs.at[s], sem_gr.at[me], "member", p).start()
    e_recv[:, me] = e_send[me]

    g_part = g_acc[...] / gain[...]
    for p in range(n):
        t_send[p, :, pl.ds(2 * d, d)] = g_part
    for s in order:
        p = peer(s)
        remote(t_send.at[p], t_recv.at[me], sem_ts.at[s], sem_tr.at[me], "member", p).start()
    t_recv[me] = t_send[me]

    unit = b_acc[...] * gain[...]
    normed = normed_ref[...]
    term = cot[...].astype(F32) + inv_ref[...] * (
        unit
        - jnp.mean(unit, axis=1, keepdims=True)
        - normed * jnp.mean(unit * normed, axis=1, keepdims=True)
    )
    term = term.astype(BF16)
    for p in range(n):
        u_send[p] = term[:, p * ds:(p + 1) * ds]
    for s in order:
        p = peer(s)
        remote(u_send.at[p], u_recv.at[me], sem_us.at[s], sem_ur.at[me], "member", p).start()

    red_s.mid(0)
    red_s.mid(1)
    if chain:
        red_s.mid(2)
        red_s.fin(0)

    for s in order:
        p = peer(s)
        remote(t_send.at[p], t_recv.at[p], sem_ts.at[s], sem_tr.at[p], "member", p).wait_recv()
    t_sum[0, :, pl.ds(0, 3 * d)] = sum(t_recv[p, :, pl.ds(0, 3 * d)] for p in range(n))
    for p in range(n):
        t_sum[0, :, pl.ds(3 * d + p * fs, fs)] = t_recv[p, :, pl.ds(3 * d, fs)]
        t_sum[0, :, pl.ds(3 * d + ff + p * fs, fs)] = t_recv[p, :, pl.ds(3 * d + fs, fs)]
    red_t.start(0)

    for s in order:
        p = peer(s)
        remote(e_send.at[p], e_recv.at[:, p], sem_gs.at[s], sem_gr.at[p], "member", p).wait_recv()
    if chain:
        for q in range(nz):
            red_e.start(q)
        red_s.mid(3)
        red_s.fin(1)
        red_t.mid(0)
        red_s.fin(2)
        red_s.fin(3)
        red_e.mid(0)
        red_t.fin(0)
        red_e.mid(1)
    else:
        red_s.plain()
        red_t.plain()
        red_e.plain()

    total = u_send[me].astype(F32)
    for s in order:
        p = peer(s)
        remote(u_send.at[p], u_recv.at[p], sem_us.at[s], sem_ur.at[p], "member", p).wait_recv()
        total += u_recv[p].astype(F32)
    o_trunk[...] = total.astype(BF16)

    if chain:
        red_e.mid(2)
        red_e.fin(0)
        red_e.mid(3)
        red_e.fin(1)
        red_e.fin(2)
        red_e.fin(3)
        for q in range(nz):
            red_s.end(q)
        red_t.end(0)
    o_shrink[...] = s_fin[...]
    o_small[...] = t_fin[0]
    if chain:
        for q in range(nz):
            red_e.end(q)
            o_expand[q] = e_fin[q]
            red_s.sent(q)
            red_e.sent(q)
        red_t.sent(0)
    else:
        o_expand[...] = e_fin[...]

    for s in order:
        p = peer(s)
        sc_cp(s).wait_send()
        e_cp(s).wait_send()
        remote(e_send.at[p], e_recv.at[:, me], sem_gs.at[s], sem_gr.at[me], "member", p).wait_send()
        remote(t_send.at[p], t_recv.at[me], sem_ts.at[s], sem_tr.at[me], "member", p).wait_send()
        remote(u_send.at[p], u_recv.at[me], sem_us.at[s], sem_ur.at[me], "member", p).wait_send()
    for s, h in own_sends:
        own_cp(s, h).wait_send()
    if square:
        fwd_cp(peer(2), 0, 4, sem_fs.at[0]).wait_send()
        fwd_cp(peer(4), 1, 2, sem_fs.at[1]).wait_send()
    for s in range(2, n, 2):
        for h in range(2):
            fwd_cp(peer(s), h, 1, sem_ps.at[s, h]).wait_send()


def finish(n, nz, trunk, expand, shrink, small, o_trunk, o_expand, o_shrink, o_in, o_hid, o_act, o_out, o_gain):
    d, ff = o_in.shape[1], o_hid.shape[1]
    ez, rz, fs = expand.shape[2], shrink.shape[1], expand.shape[3]
    o_trunk[...] = trunk[...]
    o_in[...] = small[:, pl.ds(0, d)]
    o_out[...] = small[:, pl.ds(d, d)]
    o_gain[...] = small[:, pl.ds(2 * d, d)]
    o_hid[...] = small[:, pl.ds(3 * d, ff)]
    o_act[...] = small[:, pl.ds(3 * d + ff, ff)]
    for q in range(nz):
        o_shrink[pl.ds(q * rz, rz), :] = shrink[q].astype(F32)
        for p in range(n):
            o_expand[pl.ds(q * ez, ez), pl.ds(p * fs, fs)] = expand[q, p].astype(F32)


def body(n, nz, trunk, normgain, expand, shrink, inscale, hidscale, actscale, outscale, cotangent):
    tok, d = trunk.shape
    ff = expand.shape[1]
    fs, ds = ff // n, d // n
    rz, ez = fs // nz, ds // nz
    width = 2 * d + 2 * ff
    V = pltpu.VMEM
    DMA = pltpu.SemaphoreType.DMA
    small, small2 = 3 * d + 2 * fs, 3 * d + 2 * ff

    def buffers(shape, dtype):
        first = shape if nz == 4 else (nz, *shape)
        return V(first, dtype), V(shape, dtype), V(shape, dtype), V(shape, dtype)

    parts = pl.pallas_call(
        functools.partial(kernel, n, nz),
        out_shape=[
            jax.ShapeDtypeStruct((tok, ds), BF16),
            jax.ShapeDtypeStruct((nz, n, ez, fs), BF16),
            jax.ShapeDtypeStruct((nz, rz, d), BF16),
            jax.ShapeDtypeStruct((1, small2), F32),
        ],
        in_specs=[pl.BlockSpec(memory_space=V)] * 9,
        out_specs=[pl.BlockSpec(memory_space=V)] * 4,
        scratch_shapes=[
            V((1, width), F32), V((n, ds, fs), BF16), V((fs, d), BF16), V((n, 1, width), F32),
            V((n, tok, d), BF16), V((n, tok, d), BF16),
            V((n, tok, fs), F32), V((n, tok, fs), F32), V((n, tok, fs), F32), V((n, tok, fs), BF16),
            V((tok, d), F32), V((tok, 1), F32),
            V((tok, d), F32), V((fs, d), F32), V((fs, d), F32), V((1, d), F32),
            V((n, nz, ez, fs), BF16), V((nz, n, ez, fs), BF16), V((nz, rz, d), BF16), V((1, 1, small2), F32),
            V((n, tok, ds), BF16), V((n, tok, ds), BF16),
            V((n, 1, small), F32), V((n, 1, small), F32),
            *buffers((nz, rz, d), BF16), *buffers((nz, n, ez, fs), BF16), *buffers((1, 1, small2), F32),
            DMA((n,)), DMA((n,)), DMA((n,)), DMA((n,)), DMA((n, 2)), DMA((n, 2)), DMA((2,)), DMA((n, 2)),
            DMA((n,)), DMA((n,)), DMA((n,)), DMA((n,)), DMA((n,)), DMA((n,)),
            DMA((6, nz)), DMA((6, nz)), DMA((6, nz)),
        ],
        compiler_params=pltpu.CompilerParams(
            collective_id=0, has_side_effects=True, vmem_limit_bytes=64000 * 1024
        ),
    )(trunk, normgain[None], expand, shrink, inscale, outscale, hidscale, actscale, cotangent[0])
    out = pl.pallas_call(
        functools.partial(finish, n, nz),
        out_shape=[
            jax.ShapeDtypeStruct((tok, ds), BF16),
            jax.ShapeDtypeStruct((ds, ff), F32),
            jax.ShapeDtypeStruct((fs, d), F32),
            jax.ShapeDtypeStruct((1, d), F32),
            jax.ShapeDtypeStruct((1, ff), F32),
            jax.ShapeDtypeStruct((1, ff), F32),
            jax.ShapeDtypeStruct((1, d), F32),
            jax.ShapeDtypeStruct((1, d), F32),
        ],
        in_specs=[pl.BlockSpec(memory_space=V)] * 4,
        out_specs=[pl.BlockSpec(memory_space=V)] * 8,
    )(*parts)
    o_trunk, o_expand, o_shrink, o_in, o_hid, o_act, o_out, o_gain = out
    return (o_trunk, o_expand, o_shrink, o_in, o_hid, o_act, o_out, o_gain[0])


def fast_kernel(names, cuts, *refs):
    r = dict(zip(names, refs))
    trunk, gain, expand, shrink, cot = (r[k] for k in ("trunk", "gain", "expand", "shrink", "cot"))
    me = lax.axis_index("member")
    mz = lax.axis_index("dp")
    n, nz = 8, 4
    tok, d = trunk.shape
    ff = expand.shape[1]
    fs, ds = ff // n, d // n
    chunks = len(cuts)
    offs = [sum(cuts[:c]) for c in range(chunks)]
    top = tok // 32 * 16
    rows = (pl.ds(0, top), pl.ds(top, tok - top))
    core, xx, yy = me % 2, (me // 2) % 2, me // 4

    def peer(s):
        return (((yy + s // 4) % 2) * 2 + (xx + s // 2) % 2) * 2 + (core + s) % 2

    def remote(src, dst, ss, rs, axis, who):
        return pltpu.make_async_remote_copy(
            src_ref=src, dst_ref=dst, send_sem=ss, recv_sem=rs,
            device_id={axis: who}, device_id_type=MESH,
        )

    sc_send, sc_all, e_all, et = r["sc_send"], r["sc_all"], r["e_all"], r["et"]
    for p in range(n):
        sc_send[p, :, pl.ds(0, d)] = r["r_in"][...]
        sc_send[p, :, pl.ds(d, d)] = r["r_out"][...]
        sc_send[p, :, pl.ds(2 * d, fs)] = r["r_hid"][:, p * fs:(p + 1) * fs]
        sc_send[p, :, pl.ds(2 * d + fs, fs)] = r["r_act"][:, p * fs:(p + 1) * fs]

    barrier = pltpu.get_barrier_semaphore()
    for s in range(1, n):
        pl.semaphore_signal(barrier, inc=1, device_id={"member": peer(s)}, device_id_type=MESH)
    for k in range(1, nz):
        pl.semaphore_signal(barrier, inc=1, device_id={"dp": (mz + k) % nz}, device_id_type=MESH)
    pl.semaphore_wait(barrier, n - 1 + nz - 1)

    def e_cp(s):
        p = peer(s)
        return remote(
            expand.at[:, pl.ds(pl.multiple_of(p * fs, fs), fs)], e_all.at[me],
            r["sem_es"].at[s], r["sem_er"].at[me], "member", p)

    def sc_cp(s):
        p = peer(s)
        return remote(sc_send.at[p], sc_all.at[me], r["sem_ss"].at[s], r["sem_sr"].at[me], "member", p)

    def cots(c):
        return r[f"cots{c}"]

    def own_cp(c, s, h):
        return remote(
            cot.at[rows[h], pl.ds(offs[c], cuts[c])], cots(c).at[me, rows[h]],
            r["sem_cs"].at[c, s, h], r["sem_cr"].at[c, me, h], "member", peer(s))

    def fwd_cp(c, m, h, s, sem):
        part = cots(c).at[m, rows[h]]
        return remote(part, part, sem, r["sem_cr"].at[c, m, h], "member", peer(s))

    def cross(c, h):
        a, b = ((2, 4), (4, 2))[h]
        return fwd_cp(c, peer(a), h, b, r["sem_fs"].at[c, h])

    def near(c, s, h):
        return fwd_cp(c, peer(s), h, 1, r["sem_ps"].at[c, s, h])

    def cot_wait(c, m, h):
        fwd_cp(c, m, h, 1, r["sem_fs"].at[c, 0]).wait_recv()

    def own_far(c):
        for h in range(2):
            own_cp(c, 2, h).start()
            own_cp(c, 4, 1 - h).start()

    def relay(c):
        cot_wait(c, peer(2), 0)
        cross(c, 0).start()
        cot_wait(c, peer(4), 1)
        cross(c, 1).start()
        if c + 2 < chunks:
            own_far(c + 2)

    order = [2, 4, 3, 5, 6, 7, 1]
    for s in order:
        sc_cp(s).start()
    for s in order:
        e_cp(s).start()
    for c in range(chunks):
        for h in range(2):
            own_cp(c, 1, h).start()
    for c in range(min(2, chunks)):
        own_far(c)

    e_all[me] = expand[:, pl.ds(pl.multiple_of(me * fs, fs), fs)]
    sc_all[me] = sc_send[me]
    for c in range(chunks):
        cots(c)[me] = cot[:, offs[c]:offs[c] + cuts[c]]

    normed_ref, inv_ref = r["normed"], r["inv"]
    tokens = trunk[...].astype(F32)
    centered = tokens - jnp.mean(tokens, axis=1, keepdims=True)
    inv = lax.rsqrt(jnp.mean(centered * centered, axis=1, keepdims=True) + eps)
    normed_ref[...] = centered * inv
    inv_ref[...] = inv
    s_acc, e_acc, b_acc, g_acc = r["s_acc"], r["e_acc"], r["b_acc"], r["g_acc"]
    s_acc[...] = jnp.zeros_like(s_acc)
    e_acc[...] = jnp.zeros_like(e_acc)
    b_acc[...] = jnp.zeros_like(b_acc)
    g_acc[...] = jnp.zeros_like(g_acc)

    for s in order:
        p = peer(s)
        remote(sc_send.at[p], sc_all.at[p], r["sem_ss"].at[s], r["sem_sr"].at[p], "member", p).wait_recv()

    si_all, sa_all = r["si_all"], r["sa_all"]
    proj_all, act_all, slope_all, bact = r["proj_all"], r["act_all"], r["slope_all"], r["bact"]

    @pl.loop(0, n)
    def _(s):
        s_in = sc_all[peer(s), :, pl.ds(0, d)]
        si_all[s] = (normed_ref[...] * gain[...] * s_in).astype(BF16)

    for s in order:
        p = peer(s)
        remote(e_all.at[p], e_all.at[p], r["sem_es"].at[s], r["sem_er"].at[p], "member", p).wait_recv()
    et[...] = e_all[...].reshape(d, fs).T

    @pl.loop(0, n)
    def _(s):
        @pl.when(s == RELAY_AT)
        def _():
            relay(0)

        m = peer(s)
        s_hid = sc_all[m, :, pl.ds(2 * d, fs)]
        s_act = sc_all[m, :, pl.ds(2 * d + fs, fs)]
        proj = dot(si_all[s], e_all[...].reshape(d, fs), 1, 0)
        active, slope = gelu_pair(proj * s_hid)
        proj_all[s] = proj
        act_all[s] = active
        slope_all[s] = slope * s_act
        sa_all[s] = (active * s_act).astype(BF16)

    inner = (mz == 1) | (mz == 2)
    outer = (mz == 0) | (mz == 3)
    pair = mz + 1 - 2 * (mz % 2)
    across = 3 - mz

    class Chain:
        def __init__(self, refs, sem):
            self.refs, self.sem = refs, sem

        def hop(self, k):
            own, in1, part, in2, fin = self.refs
            src, dst, who = ((own, in1, pair), (part, in2, across), (fin, fin, pair))[k]
            return remote(src, dst, self.sem(2 * k), self.sem(2 * k + 1), "dp", who)

        def start(self):
            @pl.when(outer)
            def _():
                self.hop(0).start()

        def mid(self):
            own, in1, part, in2, fin = self.refs

            @pl.when(inner)
            def _():
                self.hop(0).wait_recv()
                part[...] = (own[...].astype(F32) + in1[...].astype(F32)).astype(part.dtype)
                self.hop(1).start()

        def fin(self):
            own, in1, part, in2, fin = self.refs

            @pl.when(inner)
            def _():
                self.hop(1).wait_recv()
                fin[...] = (part[...].astype(F32) + in2[...].astype(F32)).astype(fin.dtype)
                self.hop(2).start()

        def end(self):
            @pl.when(outer)
            def _():
                self.hop(2).wait_recv()

        def sent(self):
            @pl.when(outer)
            def _():
                self.hop(0).wait_send()

            @pl.when(inner)
            def _():
                self.hop(1).wait_send()
                self.hop(2).wait_send()

    red_s = [
        Chain([r[f"s{k}_{c}"] for k in range(5)], lambda i, c=c: r["sem_zs"].at[i, c])
        for c in range(chunks)
    ]
    red_e = [
        Chain([r[f"e{k}"].at[peer(s)] for k in range(5)], lambda i, s=s: r["sem_ze"].at[i, s])
        for s in range(n)
    ]
    red_t = Chain([r[f"t{k}"] for k in range(5)], lambda i: r["sem_zt"].at[i])

    t_send, bp_all = r["t_send"], r["bp_all"]
    for c in range(chunks):
        cols = pl.ds(offs[c], cuts[c])
        last = c == chunks - 1

        @pl.loop(0, n)
        def _(s):
            m = peer(s)

            @pl.when(s == 2)
            def _():
                cot_wait(c, peer(2), 1)
                cot_wait(c, peer(4), 0)
                for a in (2, 4):
                    for h in range(2):
                        near(c, a, h).start()

            @pl.when(s == 6)
            def _():
                if not last:
                    relay(c + 1)
                if c >= 1:
                    red_s[c - 1].mid()
                if c >= 2:
                    red_s[c - 2].fin()
                for h in range(2):
                    cot_wait(c, peer(6), h)
                    near(c, 6, h).start()

            @pl.when(s % 2 == 1)
            def _():
                cot_wait(c, m, 0)
                cot_wait(c, m, 1)

            s_out = sc_all[m, :, pl.ds(d + offs[c], cuts[c])]
            scaled_cot = (cots(c)[m].astype(F32) * s_out).astype(BF16)
            back_act = dot(scaled_cot, shrink[:, cols], 1, 1)
            s_term = dot(sa_all[s], scaled_cot, 0, 0)
            s_acc[:, cols] += s_term
            t_send[m, :, pl.ds(d + offs[c], cuts[c])] = (
                jnp.sum(s_term * shrink[:, cols].astype(F32), axis=0, keepdims=True) / s_out)
            if c:
                back_act = back_act + bact[s]
            if not last:
                bact[s] = back_act
            else:
                s_in = sc_all[m, :, pl.ds(0, d)]
                s_hid = sc_all[m, :, pl.ds(2 * d, fs)]
                g_act = jnp.sum(back_act * act_all[s], axis=0, keepdims=True)
                back_hid = back_act * slope_all[s]
                g_hid = jnp.sum(back_hid * proj_all[s], axis=0, keepdims=True)
                back_proj = (back_hid * s_hid).astype(BF16)
                bp_all[s] = back_proj
                e_term = dot(back_proj, si_all[s], 0, 0)
                e_acc[...] += e_term
                e_sum = jnp.sum(e_term * et[...].astype(F32), axis=0, keepdims=True)
                g_acc[...] += e_sum
                t_send[m, :, pl.ds(0, d)] = e_sum / s_in
                t_send[m, :, pl.ds(3 * d, fs)] = g_hid
                t_send[m, :, pl.ds(3 * d + fs, fs)] = g_act

        r[f"s0_{c}"][...] = s_acc[:, cols].astype(BF16)
        red_s[c].start()

    e_send, e_recv, t_recv = r["e_send"], r["e0"], r["t_recv"]
    u_send, u_recv = r["u_send"], r["u_recv"]

    def ge_cp(s):
        p = peer(s)
        return remote(e_send.at[p], e_recv.at[me], r["sem_gs"].at[s], r["sem_gr"].at[me], "member", p)

    def ge_wait(s):
        p = peer(s)
        remote(e_send.at[p], e_recv.at[p], r["sem_gs"].at[s], r["sem_gr"].at[p], "member", p).wait_recv()

    def t_cp(s):
        p = peer(s)
        return remote(t_send.at[p], t_recv.at[me], r["sem_ts"].at[s], r["sem_tr"].at[me], "member", p)

    def u_cp(s):
        p = peer(s)
        return remote(u_send.at[p], u_recv.at[me], r["sem_us"].at[s], r["sem_ur"].at[me], "member", p)

    e_send[...] = e_acc[...].astype(BF16).T.reshape(n, ds, fs)
    tail = [1, 2, 4, 3, 5, 6, 7]
    for s in tail:
        ge_cp(s).start()
    e_recv[me] = e_send[me]
    red_e[0].start()

    g_part = g_acc[...] / gain[...]
    for p in range(n):
        t_send[p, :, pl.ds(2 * d, d)] = g_part
    for s in tail:
        t_cp(s).start()
    t_recv[me] = t_send[me]

    def back_loop(lo, hi):
        @pl.loop(lo, hi)
        def _(s):
            s_in = sc_all[peer(s), :, pl.ds(0, d)]
            b_acc[...] += dot(bp_all[s], et[...], 1, 0) * s_in

    back_loop(0, n // 2)
    ge_wait(1)
    red_e[1].start()
    back_loop(n // 2, n)

    unit = b_acc[...] * gain[...]
    normed = normed_ref[...]
    term = cot[...].astype(F32) + inv_ref[...] * (
        unit
        - jnp.mean(unit, axis=1, keepdims=True)
        - normed * jnp.mean(unit * normed, axis=1, keepdims=True)
    )
    term = term.astype(BF16)
    for p in range(n):
        u_send[p] = term[:, p * ds:(p + 1) * ds]
    for s in tail:
        u_cp(s).start()

    if chunks > 1:
        red_s[chunks - 2].fin()
    red_s[chunks - 1].mid()
    red_e[0].mid()
    for s in (2, 4):
        ge_wait(s)
        red_e[s].start()
    red_e[1].mid()
    for s in tail:
        p = peer(s)
        remote(t_send.at[p], t_recv.at[p], r["sem_ts"].at[s], r["sem_tr"].at[p], "member", p).wait_recv()
    t_sum = r["t0"]
    t_sum[:, pl.ds(0, 3 * d)] = sum(t_recv[p, :, pl.ds(0, 3 * d)] for p in range(n))
    for p in range(n):
        t_sum[:, pl.ds(3 * d + p * fs, fs)] = t_recv[p, :, pl.ds(3 * d, fs)]
        t_sum[:, pl.ds(3 * d + ff + p * fs, fs)] = t_recv[p, :, pl.ds(3 * d + fs, fs)]
    red_t.start()
    for s in (3, 5):
        ge_wait(s)
        red_e[s].start()
    red_s[chunks - 1].fin()
    red_e[0].fin()
    red_e[2].mid()
    red_e[1].fin()
    red_e[4].mid()
    for s in (6, 7):
        ge_wait(s)
        red_e[s].start()
    red_e[2].fin()
    red_t.mid()
    red_e[3].mid()
    red_e[4].fin()
    red_e[5].mid()
    red_t.fin()
    red_e[3].fin()
    red_e[6].mid()
    red_e[5].fin()
    red_e[7].mid()

    total = u_send[me].astype(F32)
    for s in tail:
        p = peer(s)
        remote(u_send.at[p], u_recv.at[p], r["sem_us"].at[s], r["sem_ur"].at[p], "member", p).wait_recv()
        total += u_recv[p].astype(F32)
    r["o_trunk"][...] = total.astype(BF16)

    red_e[6].fin()
    red_e[7].fin()
    for c in range(chunks):
        red_s[c].end()
        r["o_shrink"][:, pl.ds(offs[c], cuts[c])] = r[f"s4_{c}"][...]
    red_t.end()
    r["o_small"][...] = r["t4"][...]
    for s in (0, 1, 2, 4, 3, 5, 6, 7):
        red_e[s].end()
        r["o_expand"][peer(s)] = r["e4"][peer(s)]

    for chain in (*red_s, *red_e, red_t):
        chain.sent()
    for s in order:
        for copy in (sc_cp, e_cp, ge_cp, t_cp, u_cp):
            copy(s).wait_send()
    for c in range(chunks):
        for h in range(2):
            for s in (1, 2, 4):
                own_cp(c, s, h).wait_send()
            cross(c, h).wait_send()
            for s in (2, 4, 6):
                near(c, s, h).wait_send()


def fast_finish(n, trunk, expand, shrink, small, o_trunk, o_expand, o_shrink, o_in, o_hid, o_act, o_out, o_gain):
    d, ff = o_in.shape[1], o_hid.shape[1]
    fs = expand.shape[2]
    o_trunk[...] = trunk[...]
    o_in[...] = small[:, pl.ds(0, d)]
    o_out[...] = small[:, pl.ds(d, d)]
    o_gain[...] = small[:, pl.ds(2 * d, d)]
    o_hid[...] = small[:, pl.ds(3 * d, ff)]
    o_act[...] = small[:, pl.ds(3 * d + ff, ff)]
    o_shrink[...] = shrink[...].astype(F32)
    for p in range(n):
        o_expand[:, pl.ds(p * fs, fs)] = expand[p].astype(F32)


def fast_body(trunk, normgain, expand, shrink, inscale, hidscale, actscale, outscale, cotangent):
    n = 8
    tok, d = trunk.shape
    ff = expand.shape[1]
    fs, ds = ff // n, d // n
    cuts = [d * part // sum(PARTS) for part in PARTS]
    chunks = len(cuts)
    V = pltpu.VMEM
    DMA = pltpu.SemaphoreType.DMA
    width, small, small2 = 2 * d + 2 * fs, 3 * d + 2 * fs, 3 * d + 2 * ff
    args = ["trunk", "gain", "expand", "shrink", "r_in", "r_out", "r_hid", "r_act", "cot"]
    outs = ["o_trunk", "o_expand", "o_shrink", "o_small"]
    scratch = dict(
        sc_send=V((n, 1, width), F32), sc_all=V((n, 1, width), F32),
        e_all=V((n, ds, fs), BF16), et=V((fs, d), BF16),
        si_all=V((n, tok, d), BF16), sa_all=V((n, tok, fs), BF16), bp_all=V((n, tok, fs), BF16),
        proj_all=V((n, tok, fs), F32), act_all=V((n, tok, fs), F32), slope_all=V((n, tok, fs), F32),
        bact=V((n, tok, fs), F32),
        normed=V((tok, d), F32), inv=V((tok, 1), F32),
        b_acc=V((tok, d), F32), s_acc=V((fs, d), F32), e_acc=V((fs, d), F32), g_acc=V((1, d), F32),
        e_send=V((n, ds, fs), BF16),
        t_send=V((n, 1, small), F32), t_recv=V((n, 1, small), F32),
        u_send=V((n, tok, ds), BF16), u_recv=V((n, tok, ds), BF16),
        sem_es=DMA((n,)), sem_er=DMA((n,)), sem_ss=DMA((n,)), sem_sr=DMA((n,)),
        sem_cs=DMA((chunks, n, 2)), sem_cr=DMA((chunks, n, 2)), sem_fs=DMA((chunks, 2)), sem_ps=DMA((chunks, n, 2)),
        sem_gs=DMA((n,)), sem_gr=DMA((n,)), sem_ts=DMA((n,)), sem_tr=DMA((n,)), sem_us=DMA((n,)), sem_ur=DMA((n,)),
        sem_zs=DMA((6, chunks)), sem_ze=DMA((6, n)), sem_zt=DMA((6,)),
    )
    for c in range(chunks):
        scratch[f"cots{c}"] = V((n, tok, cuts[c]), BF16)
    for k in range(5):
        scratch[f"e{k}"] = V((n, ds, fs), BF16)
        scratch[f"t{k}"] = V((1, small2), F32)
        for c in range(chunks):
            scratch[f"s{k}_{c}"] = V((fs, cuts[c]), BF16)
    parts = pl.pallas_call(
        functools.partial(fast_kernel, [*args, *outs, *scratch], cuts),
        out_shape=[
            jax.ShapeDtypeStruct((tok, ds), BF16),
            jax.ShapeDtypeStruct((n, ds, fs), BF16),
            jax.ShapeDtypeStruct((fs, d), BF16),
            jax.ShapeDtypeStruct((1, small2), F32),
        ],
        in_specs=[pl.BlockSpec(memory_space=V)] * 9,
        out_specs=[pl.BlockSpec(memory_space=V)] * 4,
        scratch_shapes=list(scratch.values()),
        compiler_params=pltpu.CompilerParams(
            collective_id=0, has_side_effects=True, vmem_limit_bytes=VMEM_LIMIT
        ),
    )(trunk, normgain[None], expand, shrink, inscale, outscale, hidscale, actscale, cotangent[0])
    out = pl.pallas_call(
        functools.partial(fast_finish, n),
        out_shape=[
            jax.ShapeDtypeStruct((tok, ds), BF16),
            jax.ShapeDtypeStruct((ds, ff), F32),
            jax.ShapeDtypeStruct((fs, d), F32),
            jax.ShapeDtypeStruct((1, d), F32),
            jax.ShapeDtypeStruct((1, ff), F32),
            jax.ShapeDtypeStruct((1, ff), F32),
            jax.ShapeDtypeStruct((1, d), F32),
            jax.ShapeDtypeStruct((1, d), F32),
        ],
        in_specs=[pl.BlockSpec(memory_space=V)] * 4,
        out_specs=[pl.BlockSpec(memory_space=V)] * 8,
    )(*parts)
    o_trunk, o_expand, o_shrink, o_in, o_hid, o_act, o_out, o_gain = out
    return (o_trunk, o_expand, o_shrink, o_in, o_hid, o_act, o_out, o_gain[0])


def solution(mesh):
    n, nz = mesh.shape["member"], mesh.shape["dp"]
    return jax.shard_map(
        fast_body if (n, nz) == (8, 4) else functools.partial(body, n, nz),
        mesh=mesh,
        in_specs=(
            P("dp", None),
            P(),
            P("member", None),
            P("member", None),
            P("member", None),
            P("member", None),
            P("member", None),
            P("member", None),
            P("member", "dp", None),
        ),
        out_specs=(
            P("dp", "member"),
            P("member", None),
            P("member", None),
            P("member", None),
            P("member", None),
            P("member", None),
            P("member", None),
            P(),
        ),
        check_vma=False,
    )
```
